512 devices in a mesh: section: 8 (over x, y_hi), expert: 16 (over z), shard: 4 (over y_lo, core).
Axes of the slice: x: 4, y: 4 (y_hi: 2, y_lo: 2; y = y_hi * 2 + y_lo), z: 16, core: 2. Of those that a mesh axis runs over, the one named last changes fastest.
Arguments:
- fwd_in: bfloat16 [8, 2048, 3584], P('section', 'expert', 'shard'), may hold values from -6 to 6
- saved_in: bfloat16 [8, 2048, 3584], P('section', 'expert', 'shard'), may hold values from -6 to 6
- grad_in: bfloat16 [8, 2048, 3584], P('section', 'expert', 'shard'), may hold values from -6 to 6
- w_in: bfloat16 [8, 16, 3584, 1024], P('section', 'expert', 'shard'), may hold values from -0.09375 to 0.09375
- w_out: bfloat16 [8, 16, 1024, 3584], P('section', 'expert', None, 'shard'), may hold values from -0.1875 to 0.1875
- ids_fwd: int32 [8, 2048, 2], P('section', 'expert'), may hold values from 0 to 15, all different within a row; in each aligned block of 128 rows (0 to 127, 128 to 255, ..., all dimensions but the last counted through in order) at most 20 rows name the same one
- weight_fwd: int32 [8, 2048, 2], P('section', 'expert'), may hold values from 3277 to 65535
- ids_bwd: int32 [8, 2048, 2], P('section', 'expert'), may hold values from 0 to 15, all different within a row; in each aligned block of 128 rows (0 to 127, 128 to 255, ..., all dimensions but the last counted through in order) at most 20 rows name the same one
- weight_bwd: int32 [8, 2048, 2], P('section', 'expert'), may hold values from 3277 to 65535
Outputs:
- fwd_out: bfloat16 [8, 2048, 3584], P('section', 'expert', 'shard')
- bwd_out: bfloat16 [8, 2048, 3584], P('section', 'expert', 'shard')
The draws below stay inside these ranges and needn't reach their ends.
Inputs may be any that keep to these rules, and one draw needn't show every extreme that they name: `ids_fwd`: the 2 experts of a token differ. In each layer, among the 128 tokens of one index of the expert axis, no expert is chosen by more than 20 slots. `ids_bwd`: the 2 experts of a token differ. In each layer, among the 128 tokens of one index of the expert axis, no expert is chosen by more than 20 slots.
All inputs are finite; a program needn't handle non-finite values.
Results may differ from the reference program's by a relative error of at most 0.0049.
Values may be sent and summed in bfloat16 or wider, within the bound.
No kernel may reach another device: no remote copies, remote signals or barrier semaphores. Data moves between devices by JAX's collectives and lax.ppermute only.
A program may use at most 64 MiB of HBM per device.

```python
import math
import jax
import jax.numpy as jnp
import numpy as np
from jax import lax

D = 3584
FF = 1024
TOP = 2
TOK_E = 128
EXPERTS = 16
TOKENS = 2048
LAYERS = 8
CAP = 20


def plant(result, stream_key, smallest, top_value):
    longest = result.shape.index(max(result.shape))
    spots = []
    for shift in (0, 1):
        where = [jax.random.randint(jax.random.fold_in(stream_key, axis), (), 0, length) for axis, length in enumerate(result.shape)]
        where[longest] = (where[longest] + shift) % result.shape[longest]
        spots.append(tuple(where))
    return result.at[spots[0]].set(smallest).at[spots[1]].set(top_value)


def steps_of(rng, extent, pieces, smallest, high):
    factor_of = 1.0
    for dim, parts in pieces:
        draws = jax.random.uniform(jax.random.fold_in(jax.random.fold_in(rng, 6), dim), (parts,), jnp.float32, smallest / len(pieces), high / len(pieces))
        factor_of = factor_of * jnp.repeat(jnp.exp(draws), extent[dim] // parts).reshape((-1,) + (1,) * (len(extent) - 1 - dim))
    return factor_of


def assign_block(key, own, number, rows, number_of, top, reach, skew):
    sequence = jax.random.permutation(key, number_of)
    crowded, usual = portions_of(number_of, rows * top, reach, skew, True), portions_of(number_of, rows * top, reach, skew, False)
    places = jnp.arange(number_of)

    def named(sizes, offset_by):
        used = int((sizes > 0).sum())
        fixed = max(1, used // 4)
        shifted = fixed + (places - fixed + offset_by * (used - fixed)) % max(1, number_of - fixed)
        return jnp.zeros((number_of,), jnp.int32).at[sequence[jnp.where(places < fixed, places, shifted)]].set(jnp.asarray(sizes, jnp.int32))

    sizes = jnp.where(number % 4 == 0, named(crowded, number // 4), named(usual, number - number // 4 - 1))
    mixed = jax.random.permutation(jax.random.fold_in(own, 3), number_of)
    donor, sink = mixed[0:number_of // 2 * 2:2], mixed[1:number_of // 2 * 2:2]
    room = jnp.minimum(sizes[donor] - 1, reach - sizes[sink]) // 2
    room = jnp.where((donor == sequence[0]) | (sink == sequence[0]) | (sizes[sink] == 0), 0, jnp.maximum(room, 0))
    shifted = jax.random.randint(jax.random.fold_in(own, 4), (number_of // 2,), 0, 1 << 20) % (room + 1)
    sizes = sizes.at[donor].add(-shifted).at[sink].add(shifted)
    items = jnp.searchsorted(jnp.cumsum(sizes), jnp.arange(rows * top), side="right").astype(jnp.int32)
    table = items.reshape(top, rows).T
    table = table[jax.random.permutation(jax.random.fold_in(own, 1), rows)]
    offset_by = jax.random.randint(jax.random.fold_in(own, 2), (rows, 1), 0, top)
    return jnp.take_along_axis(table, (jnp.arange(top)[None, :] + offset_by) % top, axis=1)


def portions_of(amount, total, most, lean, full):
    portions = [(1 << 20) // math.isqrt(standing ** lean) + 1 for standing in range(1, amount + 1)]
    largest = most if full else min(most, max(-(-total // amount), total * portions[0] // sum(portions)))
    least = 1 if total - largest >= amount - 1 else 0
    given, rest = [largest] + [least] * (amount - 1), total - largest - least * (amount - 1)
    while rest > 0:
        candidates = [i for i in range(1, amount) if given[i] < largest] or [i for i in range(1, amount) if given[i] < most]
        pool, left = sum([portions[i] for i in candidates]), rest
        for i in candidates:
            addition = min(most - given[i], max(1, left * portions[i] // pool), rest)
            given[i] = given[i] + addition
            rest = rest - addition
    return np.array(given)


def normal_values(stream_key, shape, width, limit, split=(), held_as=jnp.bfloat16):
    factor_of = steps_of(stream_key, shape, split, -0.22, 0.18) if split else 1.0
    drawn = jax.random.normal(stream_key, shape, jnp.float32) * width * factor_of
    return jnp.minimum(jnp.maximum(drawn, -limit), limit).astype(held_as)


def setup_inputs(seed: int = 0) -> dict:
    key_list = jax.random.split(jax.random.key(seed), 10)
    fwd_in = normal_values(key_list[0], (LAYERS, TOKENS, D), 1.0, 6.0, ((0, 8), (1, 16), (2, 4)))
    saved_in = normal_values(key_list[1], (LAYERS, TOKENS, D), 1.0, 6.0, ((0, 8), (1, 16), (2, 4)))
    grad_in = normal_values(key_list[2], (LAYERS, TOKENS, D), 1.0, 6.0, ((0, 8), (1, 16), (2, 4)))
    w_in = normal_values(key_list[3], (LAYERS, EXPERTS, D, FF), D ** -0.5, 0.09375, ((0, 8), (1, 16), (2, 4)))
    w_out = normal_values(key_list[4], (LAYERS, EXPERTS, FF, D), FF ** -0.5, 0.1875, ((0, 8), (1, 16), (3, 4)))
    ids_fwd_keys = jax.random.split(jax.random.fold_in(key_list[5], 1), LAYERS * TOKENS // TOK_E)
    ids_fwd_turns = jax.random.permutation(jax.random.fold_in(key_list[5], 3), LAYERS * TOKENS // TOK_E)
    ids_fwd = jax.vmap(lambda own, number: assign_block(jax.random.fold_in(key_list[5], 2), own, number, TOK_E, EXPERTS, TOP, CAP, 1))(ids_fwd_keys, ids_fwd_turns).reshape((LAYERS, TOKENS, TOP))
    weight_fwd = plant(jax.random.randint(key_list[6], (LAYERS, TOKENS, TOP), 3277, 65536), jax.random.fold_in(key_list[6], 1), 3277, 65535).astype(jnp.int32)
    ids_bwd_keys = jax.random.split(jax.random.fold_in(key_list[7], 1), LAYERS * TOKENS // TOK_E)
    ids_bwd_turns = jax.random.permutation(jax.random.fold_in(key_list[7], 3), LAYERS * TOKENS // TOK_E)
    ids_bwd = jax.vmap(lambda own, number: assign_block(jax.random.fold_in(key_list[7], 2), own, number, TOK_E, EXPERTS, TOP, CAP, 1))(ids_bwd_keys, ids_bwd_turns).reshape((LAYERS, TOKENS, TOP))
    weight_bwd = plant(jax.random.randint(key_list[8], (LAYERS, TOKENS, TOP), 3277, 65536), jax.random.fold_in(key_list[8], 1), 3277, 65535).astype(jnp.int32)
    return dict(fwd_in=fwd_in, saved_in=saved_in, grad_in=grad_in, w_in=w_in, w_out=w_out, ids_fwd=ids_fwd, weight_fwd=weight_fwd, ids_bwd=ids_bwd, weight_bwd=weight_bwd)


def destinations(route_ids, experts, capacity):
    tokens, slot_count = route_ids.shape
    flat_ids = route_ids.reshape(-1)
    labels = jnp.arange(experts, dtype=jnp.int32)
    onehot = (flat_ids[:, None] == labels[None, :]).astype(jnp.int32)
    before = jnp.cumsum(onehot, axis=0) - onehot
    ranking = jnp.sum(before * onehot, axis=1).astype(jnp.int32)
    return (flat_ids * capacity + ranking).reshape(tokens, slot_count).astype(jnp.int32)


def buffer_index(route_ids):
    block_count = route_ids.shape[0] // TOK_E
    grouped = route_ids.reshape(block_count, TOK_E, TOP)

    def one_block(block_ids):
        return destinations(block_ids, EXPERTS, CAP)

    inside = jax.vmap(one_block)(grouped)
    position = inside - grouped * CAP
    block_rows = jnp.arange(block_count, dtype=jnp.int32)[:, None, None]
    slot_index = grouped * (block_count * CAP) + block_rows * CAP + position
    return slot_index.reshape(route_ids.shape).astype(jnp.int32), block_count * CAP


def fill_slots(tok_rows, slot_index, per_expert):
    features = tok_rows.shape[1]
    stacked = jnp.repeat(tok_rows, TOP, axis=0)
    zero_rows = jnp.zeros((EXPERTS * per_expert, features), tok_rows.dtype)
    return zero_rows.at[slot_index.reshape(-1)].set(stacked).reshape(EXPERTS, per_expert, features)


def mix_back(tok_rows, results, slot_index, route_weight):
    picked = results.reshape(EXPERTS * results.shape[1], -1)[slot_index].astype(jnp.float32)
    slot_weight = route_weight.astype(jnp.float32) / 32768.0
    mixed = tok_rows.astype(jnp.float32) + jnp.sum(slot_weight[:, :, None] * picked, axis=1)
    return mixed.astype(jnp.bfloat16)


def forward_layer(layer_args):
    tok_rows, route_ids, route_weight, up_matrix, down_matrix = layer_args
    slot_index, per_expert = buffer_index(route_ids)
    slot_rows = fill_slots(tok_rows, slot_index, per_expert)

    def expert_pass(expert_args):
        rows_here, up_here, down_here = expert_args
        hidden = jnp.dot(rows_here, up_here, preferred_element_type=jnp.float32)
        active = jax.nn.silu(hidden).astype(jnp.bfloat16)
        return jnp.dot(active, down_here, preferred_element_type=jnp.float32).astype(jnp.bfloat16)

    results = lax.map(expert_pass, (slot_rows, up_matrix, down_matrix))
    return mix_back(tok_rows, results, slot_index, route_weight)


def backward_layer(layer_args):
    tok_rows, tok_grads, route_ids, route_weight, up_matrix, down_matrix = layer_args
    slot_index, per_expert = buffer_index(route_ids)
    slot_rows = fill_slots(tok_rows, slot_index, per_expert)
    slot_grads = fill_slots(tok_grads, slot_index, per_expert)

    def expert_pass(expert_args):
        rows_here, grads_here, up_here, down_here = expert_args
        hidden = jnp.dot(rows_here, up_here, preferred_element_type=jnp.float32)
        slope_in = jnp.dot(grads_here, down_here.T, preferred_element_type=jnp.float32)
        squash = jax.nn.sigmoid(hidden)
        slope = (slope_in * squash * (1.0 + hidden * (1.0 - squash))).astype(jnp.bfloat16)
        return jnp.dot(slope, up_here.T, preferred_element_type=jnp.float32).astype(jnp.bfloat16)

    results = lax.map(expert_pass, (slot_rows, slot_grads, up_matrix, down_matrix))
    return mix_back(tok_grads, results, slot_index, route_weight)


def reference(fwd_in, saved_in, grad_in, w_in, w_out, ids_fwd, weight_fwd, ids_bwd, weight_bwd):
    layer_outs = lax.map(forward_layer, (fwd_in, ids_fwd, weight_fwd, w_in, w_out))
    layer_grads = lax.map(backward_layer, (saved_in, grad_in, ids_bwd, weight_bwd, w_in, w_out))
    fwd_out = jnp.roll(layer_outs, 1, axis=0)
    bwd_out = jnp.roll(layer_grads, -1, axis=0)
    return fwd_out, bwd_out
```

```python
import jax
import jax.numpy as jnp
from jax import lax
from jax.sharding import PartitionSpec as P

LANES = 128


def destinations(route_ids, experts, capacity):
    tokens, slot_count = route_ids.shape
    flat_ids = route_ids.reshape(-1)
    labels = jnp.arange(experts, dtype=jnp.int32)
    onehot = (flat_ids[:, None] == labels[None, :]).astype(jnp.int32)
    before = jnp.cumsum(onehot, axis=0) - onehot
    ranking = jnp.sum(before * onehot, axis=1)
    return (flat_ids * capacity + ranking).reshape(tokens, slot_count)


def dispatch_matrix(targets, slot_total):
    labels = jnp.arange(slot_total, dtype=jnp.int32)
    hits = jnp.zeros((slot_total, targets.shape[0]), jnp.bool_)
    for column in range(targets.shape[1]):
        hits = hits | (labels[:, None] == targets[None, :, column])
    return hits.astype(jnp.bfloat16)


def exchange(chunks):
    return lax.all_to_all(chunks, "expert", split_axis=0, concat_axis=0, tiled=True)


def swapped(value, mask):
    count = lax.axis_size("shard")
    return lax.ppermute(value, "shard", [(source, source ^ mask) for source in range(count)])


def shard_sum_half(partial, core):
    half = partial.shape[-1] // 2
    low, high = partial[..., :half], partial[..., half:]
    away = jnp.where(core == 0, high, low).astype(jnp.bfloat16)
    kept = jnp.where(core == 0, low, high)
    pair = kept + swapped(away, 1).astype(jnp.float32)
    return pair + swapped(pair.astype(jnp.bfloat16), 2).astype(jnp.float32)


def both_halves(mine, core):
    other = swapped(mine, 1)
    low = jnp.where(core == 0, mine, other)
    high = jnp.where(core == 0, other, mine)
    return jnp.concatenate((low, high), axis=-1)


def mix_rows(tok_rows, targets, route_weight, returned):
    picked = returned[targets].astype(jnp.float32)
    slot_weight = route_weight.astype(jnp.float32) / 32768.0
    summed = jnp.sum(slot_weight[:, :, None] * picked, axis=1)
    return (tok_rows.astype(jnp.float32) + summed).astype(jnp.bfloat16)


def from_behind(value, axis, steps):
    count = lax.axis_size(axis)
    pairs = [(source, (source + steps) % count) for source in range(count)]
    return lax.ppermute(value, axis, pairs)


def matmul(a, b, contract):
    return lax.dot_general(a, b, ((contract[:1], contract[1:]), ((), ())), preferred_element_type=jnp.float32)


def per_device(fwd_in, saved_in, grad_in, w_in, w_out, ids_fwd, weight_fwd, ids_bwd, weight_bwd):
    peers = lax.axis_size("expert")
    core = lax.axis_index("shard") % 2
    tok_count, features = fwd_in.shape[1:]
    slot_count = ids_fwd.shape[2]
    capacity = max(2, (tok_count * slot_count * 5 + 4 * peers - 1) // (4 * peers))
    slot_total = peers * capacity
    up, down = w_in[0, 0], w_out[0, 0]
    fwd_rows, saved_rows, grad_rows = fwd_in[0], saved_in[0], grad_in[0]

    fwd_targets = destinations(ids_fwd[0], peers, capacity)
    fwd_picker = dispatch_matrix(fwd_targets, slot_total)
    fwd_packed = matmul(fwd_picker, fwd_rows, (1, 0)).astype(jnp.bfloat16)
    lane_rows = capacity * features // LANES
    fwd_got = exchange(fwd_packed.reshape(peers, lane_rows, LANES))

    bwd_targets = destinations(ids_bwd[0], peers, capacity)
    bwd_picker = dispatch_matrix(bwd_targets, slot_total).reshape(peers, capacity, tok_count)
    nothing = jnp.zeros_like(bwd_picker)
    both_picker = jnp.concatenate(
        (jnp.concatenate((bwd_picker, nothing), axis=2), jnp.concatenate((nothing, bwd_picker), axis=2)), axis=1
    ).reshape(2 * slot_total, 2 * tok_count)
    both_rows = jnp.concatenate((saved_rows, grad_rows), axis=0)
    bwd_packed = matmul(both_picker, both_rows, (1, 0)).astype(jnp.bfloat16).reshape(peers, 2 * capacity, features)
    bwd_got = exchange(bwd_packed)

    hidden = shard_sum_half(matmul(fwd_got.reshape(slot_total, features), up, (1, 0)), core)
    active = both_halves(jax.nn.silu(hidden).astype(jnp.bfloat16), core)
    fwd_results = matmul(active, down, (1, 0)).astype(jnp.bfloat16)
    fwd_back = exchange(fwd_results.reshape(peers, lane_rows, LANES)).reshape(slot_total, features)
    layer_out = mix_rows(fwd_rows, fwd_targets, weight_fwd[0], fwd_back)
    fwd_out = from_behind(layer_out, "section", 1)

    saved_slots = bwd_got[:, :capacity].reshape(slot_total, features)
    grad_slots = bwd_got[:, capacity:].reshape(slot_total, features)
    partials = jnp.stack((matmul(saved_slots, up, (1, 0)), matmul(grad_slots, down, (1, 1))))
    back_hidden, slope_in = shard_sum_half(partials, core)
    squash = jax.nn.sigmoid(back_hidden)
    slope_half = (slope_in * squash * (1.0 + back_hidden * (1.0 - squash))).astype(jnp.bfloat16)
    slope = both_halves(slope_half, core)
    bwd_results = matmul(slope, up, (1, 1)).astype(jnp.bfloat16)
    bwd_back = exchange(bwd_results.reshape(peers, lane_rows, LANES)).reshape(slot_total, features)
    layer_grad = mix_rows(grad_rows, bwd_targets, weight_bwd[0], bwd_back)
    bwd_out = from_behind(layer_grad, "section", -1)
    return (fwd_out[None], bwd_out[None])


def solution(mesh):
    rows = P("section", "expert", "shard")
    slots = P("section", "expert", None)
    in_specs = (
        rows,
        rows,
        rows,
        P("section", "expert", "shard", None),
        P("section", "expert", None, "shard"),
        slots,
        slots,
        slots,
        slots,
    )
    return jax.shard_map(per_device, mesh=mesh, in_specs=in_specs, out_specs=(rows, rows), check_vma=False)
```

```python
import jax
import jax.numpy as jnp
from jax import lax
from jax.sharding import PartitionSpec as P


LANES = 128


def destinations(route_ids, experts, capacity):
    tokens, slot_count = route_ids.shape
    flat_ids = route_ids.reshape(-1)
    labels = jnp.arange(experts, dtype=jnp.int32)
    onehot = (flat_ids[:, None] == labels[None, :]).astype(jnp.int32)
    before = jnp.cumsum(onehot, axis=0) - onehot
    ranking = jnp.sum(before * onehot, axis=1)
    return (flat_ids * capacity + ranking).reshape(tokens, slot_count)


def dispatch_matrix(targets, slot_total):
    labels = jnp.arange(slot_total, dtype=jnp.int32)
    hits = jnp.zeros((slot_total, targets.shape[0]), jnp.bool_)
    for column in range(targets.shape[1]):
        hits = hits | (labels[:, None] == targets[None, :, column])
    return hits.astype(jnp.bfloat16)


def exchange(chunks):
    return lax.all_to_all(chunks, "expert", split_axis=0, concat_axis=0, tiled=True)


def swapped(value, mask):
    count = lax.axis_size("shard")
    return lax.ppermute(value, "shard", [(source, source ^ mask) for source in range(count)])


def core_sum(partial, core):
    half = partial.shape[-1] // 2
    low, high = partial[..., :half], partial[..., half:]
    return jnp.where(core == 0, low, high) + swapped(jnp.where(core == 0, high, low), 1)


def neighbour_sum(pair):
    return pair + swapped(pair.astype(jnp.bfloat16), 2).astype(jnp.float32)


def both_halves(mine, core):
    other = swapped(mine, 1)
    low = jnp.where(core == 0, mine, other)
    high = jnp.where(core == 0, other, mine)
    return jnp.concatenate((low, high), axis=-1)


def mix_rows(tok_rows, targets, route_weight, returned):
    picked = returned[targets].astype(jnp.float32)
    slot_weight = route_weight.astype(jnp.float32) / 32768.0
    summed = jnp.sum(slot_weight[:, :, None] * picked, axis=1)
    return (tok_rows.astype(jnp.float32) + summed).astype(jnp.bfloat16)


def from_behind(value, axis, steps):
    count = lax.axis_size(axis)
    pairs = [(source, (source + steps) % count) for source in range(count)]
    return lax.ppermute(value, axis, pairs)


def matmul(a, b, contract):
    return lax.dot_general(a, b, ((contract[:1], contract[1:]), ((), ())), preferred_element_type=jnp.float32)


def per_device(fwd_in, saved_in, grad_in, w_in, w_out, ids_fwd, weight_fwd, ids_bwd, weight_bwd):
    peers = lax.axis_size("expert")
    core = lax.axis_index("shard") % 2
    tok_count, features = fwd_in.shape[1:]
    slot_count = ids_fwd.shape[2]
    capacity = max(2, (tok_count * slot_count * 5 + 4 * peers - 1) // (4 * peers))
    slot_total = peers * capacity
    lane_rows = capacity * features // LANES
    up, down = w_in[0, 0], w_out[0, 0]
    fwd_rows, saved_rows, grad_rows = fwd_in[0], saved_in[0], grad_in[0]

    fwd_targets = destinations(ids_fwd[0], peers, capacity)
    bwd_targets = destinations(ids_bwd[0], peers, capacity)
    fwd_picker = dispatch_matrix(fwd_targets, slot_total).reshape(peers, capacity, tok_count)
    bwd_picker = dispatch_matrix(bwd_targets, slot_total).reshape(peers, capacity, tok_count)
    none = jnp.zeros_like(bwd_picker)
    both_picker = jnp.concatenate(
        (jnp.concatenate((fwd_picker, none), axis=2), jnp.concatenate((none, bwd_picker), axis=2)), axis=1
    ).reshape(2 * slot_total, 2 * tok_count)
    both_rows = jnp.concatenate((fwd_rows, saved_rows), axis=0)
    both_packed = matmul(both_picker, both_rows, (1, 0)).astype(jnp.bfloat16)
    both_got = exchange(both_packed.reshape(peers, 2 * capacity, features))
    grad_packed = matmul(bwd_picker.reshape(slot_total, tok_count), grad_rows, (1, 0)).astype(jnp.bfloat16)
    grad_packed = grad_packed.reshape(peers, lane_rows, LANES)
    grad_got = exchange(grad_packed)

    partial = matmul(both_got.reshape(2 * slot_total, features), up, (1, 0))
    pair = core_sum(partial, core).reshape(peers, 2 * capacity, -1)
    hidden = neighbour_sum(pair[:, :capacity].reshape(slot_total, -1))
    active = both_halves(jax.nn.silu(hidden).astype(jnp.bfloat16), core)
    fwd_results = matmul(active, down, (1, 0)).astype(jnp.bfloat16).reshape(peers, lane_rows, LANES)
    fwd_back = exchange(fwd_results)
    back_hidden = neighbour_sum(pair[:, capacity:].reshape(slot_total, -1))

    partial_slope = matmul(grad_got.reshape(slot_total, features), down, (1, 1))
    slope_in = neighbour_sum(core_sum(partial_slope, core))
    squash = jax.nn.sigmoid(back_hidden)
    slope_half = (slope_in * squash * (1.0 + back_hidden * (1.0 - squash))).astype(jnp.bfloat16)
    slope = both_halves(slope_half, core)
    bwd_results = matmul(slope, up, (1, 1)).astype(jnp.bfloat16).reshape(peers, lane_rows, LANES)
    bwd_back = exchange(bwd_results)

    layer_out = mix_rows(fwd_rows, fwd_targets, weight_fwd[0], fwd_back.reshape(slot_total, features))
    fwd_out = from_behind(layer_out, "section", 1)
    layer_grad = mix_rows(grad_rows, bwd_targets, weight_bwd[0], bwd_back.reshape(slot_total, features))
    bwd_out = from_behind(layer_grad, "section", -1)
    return (fwd_out[None], bwd_out[None])


def solution(mesh):
    rows = P("section", "expert", "shard")
    slots = P("section", "expert", None)
    in_specs = (
        rows,
        rows,
        rows,
        P("section", "expert", "shard", None),
        P("section", "expert", None, "shard"),
        slots,
        slots,
        slots,
        slots,
    )
    return jax.shard_map(per_device, mesh=mesh, in_specs=in_specs, out_specs=(rows, rows), check_vma=False)
```

```python
import jax
import jax.numpy as jnp
from jax import lax
from jax.experimental import pallas as pl
from jax.experimental.pallas import tpu as pltpu
from jax.sharding import PartitionSpec as P


LANES = 128


SUBLANES = 8
IN_VMEM = pl.BlockSpec(memory_space=pltpu.VMEM)


def iota(shape, dim):
    return lax.broadcasted_iota(jnp.int32, shape, dim)


def ones_where(mask):
    return jnp.where(mask, 1.0, 0.0).astype(jnp.bfloat16)


def places_in_chunks(ids, experts):
    tokens = ids.shape[1]
    earlier = ones_where(iota((tokens, tokens), 0) < iota((tokens, tokens), 1))
    label = iota((experts, tokens), 0)
    first, second = (jnp.where(label == ids[column : column + 1], 1.0, 0.0) for column in range(2))
    before = matmul(jnp.concatenate((first, second), axis=0).astype(jnp.bfloat16), earlier, (1, 0))
    first_rank = jnp.sum(first * before[:experts], axis=0, keepdims=True)
    after_first = before[experts:] + jnp.sum(first, axis=1, keepdims=True)
    second_rank = jnp.sum(second * after_first, axis=0, keepdims=True)
    return first_rank.astype(jnp.int32), second_rank.astype(jnp.int32)


def in_vmem(array):
    return pltpu.with_memory_space_constraint(array, pltpu.VMEM)


def call(kernel, out_shape, *operands):
    outs = out_shape if isinstance(out_shape, tuple) else (out_shape,)
    specs = tuple(IN_VMEM for _ in outs)
    return pl.pallas_call(
        kernel,
        out_shape=out_shape,
        in_specs=[pl.BlockSpec(memory_space=pltpu.SMEM) if x.ndim == 1 else IN_VMEM for x in operands],
        out_specs=specs if isinstance(out_shape, tuple) else specs[0],
        compiler_params=pltpu.CompilerParams(vmem_limit_bytes=24 << 20),
    )(*operands)


def shaped(shape, dtype=jnp.bfloat16):
    return jax.ShapeDtypeStruct(shape, dtype)


FULL = 2 * SUBLANES


def chunk_row(rank, which):
    return jnp.where(rank < FULL, which * FULL + rank, FULL + 4 * which + rank)


def route_kernel(experts, capacity, ids_fwd, ids_bwd, fwd_rows, saved_rows, packed, targets):
    tokens = fwd_rows.shape[0]
    chosen = []
    for which, ids_ref in enumerate((ids_fwd, ids_bwd)):
        ids = ids_ref[...]
        ranks = places_in_chunks(ids, experts)
        for column in range(2):
            expert = ids[column : column + 1]
            targets[2 * which + column : 2 * which + column + 1, :] = expert * capacity + ranks[column]
            chosen.append(expert * (2 * capacity) + chunk_row(ranks[column], which))
    block = LANES
    for start in range(0, packed.shape[0], block):
        row = iota((block, tokens), 0) + start
        fwd_hits = ones_where((row == chosen[0]) | (row == chosen[1]))
        saved_hits = ones_where((row == chosen[2]) | (row == chosen[3]))
        both = matmul(fwd_hits, fwd_rows[...], (1, 0)) + matmul(saved_hits, saved_rows[...], (1, 0))
        packed[start : start + block, :] = both.astype(jnp.bfloat16)


def route_and_pack(ids_fwd, ids_bwd, fwd_rows, saved_rows, experts, capacity):
    tokens, features = fwd_rows.shape
    return call(
        lambda *refs: route_kernel(experts, capacity, *refs),
        (shaped((2 * experts * capacity, features)), shaped((4, tokens), jnp.int32)),
        ids_fwd,
        ids_bwd,
        fwd_rows,
        saved_rows,
    )


def put_tiles(out_ref, tile, last_tile):
    experts, chunk_rows, lanes = out_ref.shape
    columns = (2 * chunk_rows // SUBLANES) // 5

    def put(at, value):
        rows = slice(at * SUBLANES, (at + 1) * SUBLANES)
        out_ref[:, rows, :] = value.astype(jnp.bfloat16).reshape(experts, SUBLANES, lanes)

    for part in range(2):
        for column in range(columns):
            put(part * columns + column, tile(part, column))
    for pair in range((columns + 1) // 2):
        put(2 * columns + pair, last_tile(2 * pair, min(2 * pair + 1, columns - 1)))


def chunk_tile(tiled, at):
    experts, _, lanes = tiled.shape
    return tiled[:, at * SUBLANES : (at + 1) * SUBLANES, :].reshape(experts * SUBLANES, lanes)


def tiled_shape(experts, features):
    columns = features // LANES
    return shaped((experts, (2 * columns + (columns + 1) // 2) * SUBLANES, LANES))


def pack_kernel(capacity, targets, rows, out):
    experts = out.shape[0]
    tokens = rows.shape[0]
    width = experts * SUBLANES
    row = iota((width, tokens), 0)
    chunk, within = row // SUBLANES, row % SUBLANES
    first, second = targets[2:3, :], targets[3:4, :]

    def picks(slot, allowed):
        return ones_where(((slot == first) | (slot == second)) & allowed)

    full = [matmul(picks(chunk * capacity + part * SUBLANES + within, True), rows[...], (1, 0)) for part in range(2)]
    last = chunk * capacity + FULL + within % 4
    early = matmul(picks(last, within < 4), rows[...], (1, 0))
    late = matmul(picks(last, within >= 4), rows[...], (1, 0))

    def lanes(column):
        return slice(column * LANES, (column + 1) * LANES)

    put_tiles(out, lambda part, c: full[part][:, lanes(c)], lambda a, b: early[:, lanes(a)] + late[:, lanes(b)])


def pack_rows(targets, rows, experts, capacity):
    out = tiled_shape(experts, rows.shape[1])
    return call(lambda *refs: pack_kernel(capacity, *refs), out, targets, rows)


def columns_of(weight, contract, half):
    units = 512
    span = pl.ds(pl.multiple_of(half * units, units), units)
    return weight[span, :] if contract == 1 else weight[:, span]


def hidden_kernel(core, rows, up, away, kept):
    experts, _, features = rows.shape
    pieces = (rows[:, :FULL, :], rows[:, 2 * FULL :, :], rows[:, FULL : 2 * FULL, :])
    flat = jnp.concatenate([p.reshape(experts * p.shape[1], features) for p in pieces], axis=0)
    away[...] = matmul(flat, columns_of(up, 0, 1 - core[0]), (1, 0))
    kept[...] = matmul(flat, columns_of(up, 0, core[0]), (1, 0))


def hidden_partials(core, rows, up):
    experts, chunk, _ = rows.shape
    half = shaped((experts * chunk, up.shape[1] // 2), jnp.float32)
    return call(hidden_kernel, (half, half), core, in_vmem(rows), in_vmem(up))


def slope_kernel(core, tiled, down, away, kept):
    experts, _, lanes = tiled.shape
    columns = down.shape[1] // lanes
    width = experts * SUBLANES
    full = [jnp.concatenate([chunk_tile(tiled, p * columns + c) for c in range(columns)], axis=1) for p in range(2)]
    main = jnp.concatenate([full[p].reshape(experts, SUBLANES, -1) for p in range(2)], axis=1)
    main = main.reshape(2 * width, -1)
    lasts = [chunk_tile(tiled, 2 * columns + pair) for pair in range((columns + 1) // 2)]
    for out, half in ((away, 1 - core[0]), (kept, core[0])):
        weight = columns_of(down, 1, half)
        early = late = None
        for column in range(columns):
            part = matmul(lasts[column // 2], weight[:, column * lanes : (column + 1) * lanes], (1, 1))
            if column % 2:
                late = part if late is None else late + part
            else:
                early = part if early is None else early + part
        out[: 2 * width, :] = matmul(main, weight, (1, 1))
        out[2 * width :, :] = late + pltpu.roll(early, 4, 0)


def slope_partials(core, tiled, down):
    half = shaped((3 * tiled.shape[0] * SUBLANES, down.shape[0] // 2), jnp.float32)
    return call(slope_kernel, (half, half), core, in_vmem(tiled), in_vmem(down))


def results_kernel(contract, late_rows, core, mine, other, weight, out):
    experts, _, lanes = out.shape
    width = experts * SUBLANES
    inner = 1 - contract
    total = matmul(mine[...], columns_of(weight, inner, core[0]), (1, contract))
    total = total + matmul(other[...], columns_of(weight, inner, 1 - core[0]), (1, contract))
    main = total[: 2 * width].reshape(experts, FULL, -1)
    last = total[2 * width :]
    moved = pltpu.roll(last, width - 4 if late_rows else 4, 0)
    early, late = (moved, last) if late_rows else (last, moved)
    upper = iota((width, lanes), 0) % SUBLANES < 4

    def span(column):
        return slice(column * lanes, (column + 1) * lanes)

    put_tiles(
        out,
        lambda part, c: main[:, part * SUBLANES : (part + 1) * SUBLANES, span(c)],
        lambda a, b: jnp.where(upper, early[:, span(a)], late[:, span(b)]),
    )


def tiled_results(core, mine, other, weight, contract, late_rows, experts):
    out = tiled_shape(experts, weight.shape[1 - contract])
    kernel = lambda *refs: results_kernel(contract, late_rows, *refs)
    return call(kernel, out, core, in_vmem(mine), in_vmem(other), in_vmem(weight))


def slot_weights(targets, route_weight, experts, capacity):
    tokens = targets.shape[1]
    width = experts * SUBLANES
    expert, rank = targets // capacity, targets % capacity
    options = []
    for odd in range(2):
        last = 2 * width + expert * SUBLANES + (rank - FULL) + 4 * odd
        main = (rank // SUBLANES) * width + expert * SUBLANES + rank % SUBLANES
        options.append(jnp.where(rank < FULL, main, last))
    spots = jnp.stack(options)
    bytes_of = jnp.stack((route_weight // 256, route_weight % 256))
    labels = jnp.arange(3 * width, dtype=jnp.int32)
    hit = spots[:, :, :, None] == labels
    chosen = jnp.where(hit[:, None], bytes_of[None, :, :, :, None], 0).sum(axis=2)
    return chosen.astype(jnp.bfloat16).reshape(2, 2 * tokens, 3 * width)


def mix_kernel(weights, back, rows, out):
    tokens, features = rows.shape
    columns = features // LANES
    for column in range(columns):
        spots = (column, columns + column, 2 * columns + column // 2)
        tile = jnp.concatenate([chunk_tile(back, at) for at in spots], axis=0)
        both = matmul(weights[column % 2], tile, (1, 0))
        summed = (both[:tokens] * 256.0 + both[tokens:]) * (1.0 / 32768.0)
        lanes = slice(column * LANES, (column + 1) * LANES)
        out[:, lanes] = (rows[:, lanes].astype(jnp.float32) + summed).astype(jnp.bfloat16)


def mix(weights, back, rows):
    return call(mix_kernel, shaped(rows.shape), in_vmem(weights), in_vmem(back), in_vmem(rows))


def exchange(chunks):
    return lax.all_to_all(chunks, "expert", split_axis=0, concat_axis=0, tiled=True)


def swapped(value, mask):
    count = lax.axis_size("shard")
    return lax.ppermute(value, "shard", [(source, source ^ mask) for source in range(count)])


def rounded(value):
    return value.astype(jnp.bfloat16)


def neighbour_sum(pair):
    return pair + swapped(rounded(pair), 2).astype(jnp.float32)


def from_behind(value, axis, steps):
    count = lax.axis_size(axis)
    pairs = [(source, (source + steps) % count) for source in range(count)]
    return lax.ppermute(value, axis, pairs)


def matmul(a, b, contract):
    return lax.dot_general(a, b, ((contract[:1], contract[1:]), ((), ())), preferred_element_type=jnp.float32)


def per_device(fwd_in, saved_in, grad_in, w_in, w_out, ids_fwd, weight_fwd, ids_bwd, weight_bwd):
    peers = lax.axis_size("expert")
    core = (lax.axis_index("shard") % 2).reshape(1)
    tok_count, features = fwd_in.shape[1:]
    slot_count = ids_fwd.shape[2]
    capacity = max(2, (tok_count * slot_count * 5 + 4 * peers - 1) // (4 * peers))
    up, down = w_in[0, 0], w_out[0, 0]
    fwd_rows, saved_rows, grad_rows = fwd_in[0], saved_in[0], grad_in[0]
    full, last = peers * FULL, peers * SUBLANES

    both_packed, targets = route_and_pack(ids_fwd[0].T, ids_bwd[0].T, fwd_rows, saved_rows, peers, capacity)
    both_got = exchange(both_packed.reshape(peers, 2 * capacity, features))
    grad_packed = pack_rows(targets, grad_rows, peers, capacity)
    fwd_weights = slot_weights(targets[:2], weight_fwd[0].T, peers, capacity)
    bwd_weights = slot_weights(targets[2:], weight_bwd[0].T, peers, capacity)
    grad_got = exchange(grad_packed)

    away, kept = hidden_partials(core, both_got, up)
    pair = kept + swapped(away, 1)
    hidden = neighbour_sum(pair[: full + last])
    saved_hidden = neighbour_sum(pair[full + last :])
    active = rounded(jax.nn.silu(hidden))
    other_active = swapped(active, 1)
    fwd_results = tiled_results(core, active, other_active, down, 0, False, peers)
    fwd_back = exchange(fwd_results)

    slope_away, slope_kept = slope_partials(core, grad_got, down)
    slope_pair = slope_kept + swapped(slope_away, 1)
    slope_in = neighbour_sum(slope_pair)
    back_hidden = jnp.concatenate((saved_hidden, hidden[full:]), axis=0)
    squash = jax.nn.sigmoid(back_hidden)
    slope = rounded(slope_in * squash * (1.0 + back_hidden * (1.0 - squash)))
    other_slope = swapped(slope, 1)
    bwd_results = tiled_results(core, slope, other_slope, up, 1, True, peers)
    bwd_back = exchange(bwd_results)

    layer_out = mix(fwd_weights, fwd_back, fwd_rows)
    fwd_out = from_behind(layer_out, "section", 1)
    layer_grad = mix(bwd_weights, bwd_back, grad_rows)
    bwd_out = from_behind(layer_grad, "section", -1)
    return (fwd_out[None], bwd_out[None])


def solution(mesh):
    rows = P("section", "expert", "shard")
    slots = P("section", "expert", None)
    in_specs = (
        rows,
        rows,
        rows,
        P("section", "expert", "shard", None),
        P("section", "expert", None, "shard"),
        slots,
        slots,
        slots,
        slots,
    )
    return jax.shard_map(per_device, mesh=mesh, in_specs=in_specs, out_specs=(rows, rows), check_vma=False)
```

```python
import jax
import jax.numpy as jnp
from jax import lax
from jax.experimental import pallas as pl
from jax.experimental.pallas import tpu as pltpu
from jax.sharding import PartitionSpec as P


LANES = 128
PAUSE = 3000


SUBLANES = 8
IN_VMEM = pl.BlockSpec(memory_space=pltpu.VMEM)


def iota(shape, dim):
    return lax.broadcasted_iota(jnp.int32, shape, dim)


def ones_where(mask):
    return jnp.where(mask, 1.0, 0.0).astype(jnp.bfloat16)


def places_in_chunks(ids, experts):
    tokens = ids.shape[1]
    earlier = ones_where(iota((tokens, tokens), 0) < iota((tokens, tokens), 1))
    label = iota((experts, tokens), 0)
    first, second = (jnp.where(label == ids[column : column + 1], 1.0, 0.0) for column in range(2))
    before = matmul(jnp.concatenate((first, second), axis=0).astype(jnp.bfloat16), earlier, (1, 0))
    first_rank = jnp.sum(first * before[:experts], axis=0, keepdims=True)
    after_first = before[experts:] + jnp.sum(first, axis=1, keepdims=True)
    second_rank = jnp.sum(second * after_first, axis=0, keepdims=True)
    return first_rank.astype(jnp.int32), second_rank.astype(jnp.int32)


def in_vmem(array):
    return pltpu.with_memory_space_constraint(array, pltpu.VMEM)


def call(kernel, out_shape, *operands):
    outs = out_shape if isinstance(out_shape, tuple) else (out_shape,)
    specs = tuple(IN_VMEM for _ in outs)
    return pl.pallas_call(
        kernel,
        out_shape=out_shape,
        in_specs=[pl.BlockSpec(memory_space=pltpu.SMEM) if x.ndim == 1 else IN_VMEM for x in operands],
        out_specs=specs if isinstance(out_shape, tuple) else specs[0],
        compiler_params=pltpu.CompilerParams(vmem_limit_bytes=24 << 20),
    )(*operands)


def shaped(shape, dtype=jnp.bfloat16):
    return jax.ShapeDtypeStruct(shape, dtype)


FULL = 2 * SUBLANES


def chunk_row(rank, which):
    return jnp.where(rank < FULL, which * FULL + rank, FULL + 4 * which + rank)


def route_kernel(experts, capacity, pause, ids_fwd_hbm, ids_bwd_hbm, rows_hbm, packed, targets, held, ids_fwd, ids_bwd, rows, sems):
    copies = [
        pltpu.make_async_copy(source, target, sems.at[index])
        for index, (source, target) in enumerate(((ids_fwd_hbm, ids_fwd), (ids_bwd_hbm, ids_bwd), (rows_hbm, rows)))
    ]
    for copy in copies:
        copy.start()
    for which, ids_ref in enumerate((ids_fwd, ids_bwd)):
        copies[which].wait()
        ids = ids_ref[...]
        ranks = places_in_chunks(ids, experts)
        for column in range(2):
            row = 2 * which + column
            targets[row : row + 1, :] = ids[column : column + 1] * capacity + ranks[column]
    copies[2].wait()
    pack_tiles(capacity, targets[0:1, :], targets[1:2, :], rows[...], packed)
    held[...] = lax.fori_loop(0, pause[0], lambda _, value: value * 1.0001 + 0.5, jnp.zeros(held.shape, jnp.float32))


def route_and_pack(pause, ids_fwd, ids_bwd, rows, experts, capacity):
    tokens, features = rows.shape
    in_hbm = [pltpu.with_memory_space_constraint(x, pltpu.HBM) for x in (ids_fwd, ids_bwd, rows)]
    out_shape = (tiled_shape(experts, features), shaped((4, tokens), jnp.int32), shaped((SUBLANES, LANES), jnp.float32))
    return pl.pallas_call(
        lambda *refs: route_kernel(experts, capacity, *refs),
        out_shape=out_shape,
        in_specs=[pl.BlockSpec(memory_space=pltpu.SMEM)] + [pl.BlockSpec(memory_space=pltpu.HBM)] * 3,
        out_specs=(IN_VMEM,) * 3,
        scratch_shapes=[
            pltpu.VMEM((2, tokens), jnp.int32),
            pltpu.VMEM((2, tokens), jnp.int32),
            pltpu.VMEM((tokens, features), jnp.bfloat16),
            pltpu.SemaphoreType.DMA((3,)),
        ],
        compiler_params=pltpu.CompilerParams(vmem_limit_bytes=24 << 20),
        name="route_and_pack",
    )(pause, *in_hbm)


def pair_kernel(capacity, targets, saved_rows, grad_rows, packed):
    tokens = saved_rows.shape[0]
    spots = []
    for which in range(2):
        for column in range(2):
            slot = targets[2 + column : 3 + column, :]
            expert = lax.div(slot, jnp.int32(capacity))
            spots.append(expert * (2 * capacity) + chunk_row(slot - expert * capacity, which))
    block = LANES
    for start in range(0, packed.shape[0], block):
        row = iota((block, tokens), 0) + start
        saved_hits = ones_where((row == spots[0]) | (row == spots[1]))
        grad_hits = ones_where((row == spots[2]) | (row == spots[3]))
        both = matmul(saved_hits, saved_rows[...], (1, 0)) + matmul(grad_hits, grad_rows[...], (1, 0))
        packed[start : start + block, :] = both.astype(jnp.bfloat16)


def pack_pairs(targets, saved_rows, grad_rows, experts, capacity):
    out = shaped((2 * experts * capacity, saved_rows.shape[1]))
    kernel = lambda *refs: pair_kernel(capacity, *refs)
    return call(kernel, out, targets, saved_rows, grad_rows)


def put_tiles(out_ref, tile, last_tile):
    experts, chunk_rows, lanes = out_ref.shape
    columns = (2 * chunk_rows // SUBLANES) // 5

    def put(at, value):
        rows = slice(at * SUBLANES, (at + 1) * SUBLANES)
        out_ref[:, rows, :] = value.astype(jnp.bfloat16).reshape(experts, SUBLANES, lanes)

    for part in range(2):
        for column in range(columns):
            put(part * columns + column, tile(part, column))
    for pair in range((columns + 1) // 2):
        put(2 * columns + pair, last_tile(2 * pair, min(2 * pair + 1, columns - 1)))


def chunk_tile(tiled, at):
    experts, _, lanes = tiled.shape
    return tiled[:, at * SUBLANES : (at + 1) * SUBLANES, :].reshape(experts * SUBLANES, lanes)


def tiled_shape(experts, features):
    columns = features // LANES
    return shaped((experts, (2 * columns + (columns + 1) // 2) * SUBLANES, LANES))


def pack_tiles(capacity, first, second, rows, out):
    experts = out.shape[0]
    width = experts * SUBLANES
    row = iota((width, rows.shape[0]), 0)
    chunk, within = row // SUBLANES, row % SUBLANES

    def picks(slot, allowed):
        return ones_where(((slot == first) | (slot == second)) & allowed)

    full = [matmul(picks(chunk * capacity + part * SUBLANES + within, True), rows, (1, 0)) for part in range(2)]
    last = chunk * capacity + FULL + within % 4
    early = matmul(picks(last, within < 4), rows, (1, 0))
    late = matmul(picks(last, within >= 4), rows, (1, 0))

    def lanes(column):
        return slice(column * LANES, (column + 1) * LANES)

    put_tiles(out, lambda part, c: full[part][:, lanes(c)], lambda a, b: early[:, lanes(a)] + late[:, lanes(b)])


def columns_of(weight, contract, half):
    units = 512
    span = pl.ds(pl.multiple_of(half * units, units), units)
    return weight[span, :] if contract == 1 else weight[:, span]


def hidden_kernel(core, tiled, up, away, kept):
    experts, _, lanes = tiled.shape
    columns = up.shape[0] // lanes
    width = experts * SUBLANES
    full = [jnp.concatenate([chunk_tile(tiled, p * columns + c) for c in range(columns)], axis=1) for p in range(2)]
    main = jnp.concatenate([full[p].reshape(experts, SUBLANES, -1) for p in range(2)], axis=1)
    main = main.reshape(2 * width, -1)
    lasts = [chunk_tile(tiled, 2 * columns + pair) for pair in range((columns + 1) // 2)]
    for out, half in ((away, 1 - core[0]), (kept, core[0])):
        weight = columns_of(up, 0, half)
        early = late = None
        for column in range(columns):
            part = matmul(lasts[column // 2], weight[column * lanes : (column + 1) * lanes, :], (1, 0))
            if column % 2:
                late = part if late is None else late + part
            else:
                early = part if early is None else early + part
        out[: 2 * width, :] = matmul(main, weight, (1, 0))
        out[2 * width :, :] = early + pltpu.roll(late, width - 4, 0)


def hidden_partials(core, tiled, up):
    half = shaped((3 * tiled.shape[0] * SUBLANES, up.shape[1] // 2), jnp.float32)
    return call(hidden_kernel, (half, half), core, in_vmem(tiled), in_vmem(up))


def back_kernel(core, rows, up, down, away, kept):
    experts, _, features = rows.shape
    full, width = experts * FULL, experts * SUBLANES
    saved = rows[:, :FULL, :].reshape(full, features)
    grads = rows[:, FULL : 2 * FULL, :].reshape(full, features)
    last = rows[:, 2 * FULL :, :].reshape(width, features)
    for out, half in ((away, 1 - core[0]), (kept, core[0])):
        up_half, down_half = columns_of(up, 0, half), columns_of(down, 1, half)
        out[:full, :] = matmul(saved, up_half, (1, 0))
        out[full : 2 * full, :] = matmul(grads, down_half, (1, 1))
        upper = iota((width, out.shape[1]), 0) % SUBLANES < 4
        out[2 * full :, :] = jnp.where(upper, matmul(last, up_half, (1, 0)), matmul(last, down_half, (1, 1)))


def back_partials(core, rows, up, down):
    half = shaped((rows.shape[0] * rows.shape[1], up.shape[1] // 2), jnp.float32)
    return call(back_kernel, (half, half), core, in_vmem(rows), in_vmem(up), in_vmem(down))


def slope_kernel(width, pair, came, slope):
    full = 2 * width

    def slope_of(hidden, slope_in):
        squash = 1.0 / (1.0 + jnp.exp(-hidden))
        return (slope_in * squash * (1.0 + hidden * (1.0 - squash))).astype(jnp.bfloat16)

    total = pair[...] + came[...].astype(jnp.float32)
    slope[:full, :] = slope_of(total[:full], total[full : 2 * full])
    last = total[2 * full :]
    slope[full:, :] = slope_of(last, pltpu.roll(last, width - 4, 0))


def slopes(pair, came, experts):
    out = shaped((3 * experts * SUBLANES, pair.shape[1]))
    kernel = lambda *refs: slope_kernel(experts * SUBLANES, *refs)
    return call(kernel, out, in_vmem(pair), in_vmem(came))


def results_kernel(contract, core, mine, other, weight, out):
    experts, _, lanes = out.shape
    width = experts * SUBLANES
    inner = 1 - contract
    total = matmul(mine[...], columns_of(weight, inner, core[0]), (1, contract))
    total = total + matmul(other[...], columns_of(weight, inner, 1 - core[0]), (1, contract))
    main = total[: 2 * width].reshape(experts, FULL, -1)
    last = total[2 * width :]
    moved = pltpu.roll(last, 4, 0)
    upper = iota((width, lanes), 0) % SUBLANES < 4

    def span(column):
        return slice(column * lanes, (column + 1) * lanes)

    put_tiles(
        out,
        lambda part, c: main[:, part * SUBLANES : (part + 1) * SUBLANES, span(c)],
        lambda a, b: jnp.where(upper, last[:, span(a)], moved[:, span(b)]),
    )


def tiled_results(core, mine, other, weight, contract, experts):
    out = tiled_shape(experts, weight.shape[1 - contract])
    kernel = lambda *refs: results_kernel(contract, *refs)
    return call(kernel, out, core, in_vmem(mine), in_vmem(other), in_vmem(weight))


def slot_weights(targets, route_weight, experts, capacity):
    tokens = targets.shape[1]
    width = experts * SUBLANES
    expert, rank = targets // capacity, targets % capacity
    options = []
    for odd in range(2):
        last = 2 * width + expert * SUBLANES + (rank - FULL) + 4 * odd
        main = (rank // SUBLANES) * width + expert * SUBLANES + rank % SUBLANES
        options.append(jnp.where(rank < FULL, main, last))
    spots = jnp.stack(options)
    bytes_of = jnp.stack((route_weight // 256, route_weight % 256))
    labels = jnp.arange(3 * width, dtype=jnp.int32)
    hit = spots[:, :, :, None] == labels
    chosen = jnp.where(hit[:, None], bytes_of[None, :, :, :, None], 0).sum(axis=2)
    return chosen.astype(jnp.bfloat16).reshape(2, 2 * tokens, 3 * width)


def mix_kernel(weights, back, rows, out):
    tokens, features = rows.shape
    columns = features // LANES
    for column in range(columns):
        spots = (column, columns + column, 2 * columns + column // 2)
        tile = jnp.concatenate([chunk_tile(back, at) for at in spots], axis=0)
        both = matmul(weights[column % 2], tile, (1, 0))
        summed = (both[:tokens] * 256.0 + both[tokens:]) * (1.0 / 32768.0)
        lanes = slice(column * LANES, (column + 1) * LANES)
        out[:, lanes] = (rows[:, lanes].astype(jnp.float32) + summed).astype(jnp.bfloat16)


def mix(weights, back, rows):
    return call(mix_kernel, shaped(rows.shape), in_vmem(weights), in_vmem(back), in_vmem(rows))


def exchange(chunks):
    return lax.all_to_all(chunks, "expert", split_axis=0, concat_axis=0, tiled=True)


def swapped(value, mask):
    count = lax.axis_size("shard")
    return lax.ppermute(value, "shard", [(source, source ^ mask) for source in range(count)])


def rounded(value):
    return value.astype(jnp.bfloat16)


def from_behind(value, axis, steps):
    count = lax.axis_size(axis)
    pairs = [(source, (source + steps) % count) for source in range(count)]
    return lax.ppermute(value, axis, pairs)


def matmul(a, b, contract):
    return lax.dot_general(a, b, ((contract[:1], contract[1:]), ((), ())), preferred_element_type=jnp.float32)


def per_device(fwd_in, saved_in, grad_in, w_in, w_out, ids_fwd, weight_fwd, ids_bwd, weight_bwd):
    peers = lax.axis_size("expert")
    core = (lax.axis_index("shard") % 2).reshape(1)
    tok_count, features = fwd_in.shape[1:]
    slot_count = ids_fwd.shape[2]
    capacity = max(2, (tok_count * slot_count * 5 + 4 * peers - 1) // (4 * peers))
    up, down = w_in[0, 0], w_out[0, 0]
    fwd_rows, saved_rows, grad_rows = fwd_in[0], saved_in[0], grad_in[0]

    fwd_packed, targets, _ = route_and_pack(core * PAUSE, ids_fwd[0].T, ids_bwd[0].T, fwd_rows, peers, capacity)
    fwd_got = exchange(fwd_packed)
    bwd_packed = pack_pairs(targets, saved_rows, grad_rows, peers, capacity)
    fwd_weights = slot_weights(targets[:2], weight_fwd[0].T, peers, capacity)
    bwd_weights = slot_weights(targets[2:], weight_bwd[0].T, peers, capacity)
    bwd_got = exchange(bwd_packed.reshape(peers, 2 * capacity, features))

    away, kept = hidden_partials(core, fwd_got, up)
    pair = kept + swapped(away, 1)
    hidden = pair + swapped(rounded(pair), 2).astype(jnp.float32)
    active = rounded(jax.nn.silu(hidden))
    other_active = swapped(active, 1)
    fwd_results = tiled_results(core, active, other_active, down, 0, peers)
    fwd_back = exchange(fwd_results)

    back_away, back_kept = back_partials(core, bwd_got, up, down)
    back_pair = back_kept + swapped(back_away, 1)
    back_came = swapped(rounded(back_pair), 2)
    slope = slopes(back_pair, back_came, peers)
    other_slope = swapped(slope, 1)
    bwd_results = tiled_results(core, slope, other_slope, up, 1, peers)
    bwd_back = exchange(bwd_results)

    layer_out = mix(fwd_weights, fwd_back, fwd_rows)
    fwd_out = from_behind(layer_out, "section", 1)
    layer_grad = mix(bwd_weights, bwd_back, grad_rows)
    bwd_out = from_behind(layer_grad, "section", -1)
    return (fwd_out[None], bwd_out[None])


def solution(mesh):
    rows = P("section", "expert", "shard")
    slots = P("section", "expert", None)
    in_specs = (
        rows,
        rows,
        rows,
        P("section", "expert", "shard", None),
        P("section", "expert", None, "shard"),
        slots,
        slots,
        slots,
        slots,
    )
    return jax.shard_map(per_device, mesh=mesh, in_specs=in_specs, out_specs=(rows, rows), check_vma=False)
```

```python
import jax
import jax.numpy as jnp
from jax import lax
from jax.experimental import pallas as pl
from jax.experimental.pallas import tpu as pltpu
from jax.sharding import PartitionSpec as P


LANES = 128
PAUSE = 3000


SUBLANES = 8
IN_VMEM = pl.BlockSpec(memory_space=pltpu.VMEM)


def iota(shape, dim):
    return lax.broadcasted_iota(jnp.int32, shape, dim)


def ones_where(mask):
    return jnp.where(mask, 1.0, 0.0).astype(jnp.bfloat16)


def places_in_chunks(ids, experts):
    tokens = ids.shape[1]
    earlier = ones_where(iota((tokens, tokens), 0) < iota((tokens, tokens), 1))
    label = iota((experts, tokens), 0)
    first, second = (jnp.where(label == ids[column : column + 1], 1.0, 0.0) for column in range(2))
    before = matmul(jnp.concatenate((first, second), axis=0).astype(jnp.bfloat16), earlier, (1, 0))
    first_rank = jnp.sum(first * before[:experts], axis=0, keepdims=True)
    after_first = before[experts:] + jnp.sum(first, axis=1, keepdims=True)
    second_rank = jnp.sum(second * after_first, axis=0, keepdims=True)
    return first_rank.astype(jnp.int32), second_rank.astype(jnp.int32)


def in_vmem(array):
    return pltpu.with_memory_space_constraint(array, pltpu.VMEM)


def call(kernel, out_shape, *operands):
    outs = out_shape if isinstance(out_shape, tuple) else (out_shape,)
    specs = tuple(IN_VMEM for _ in outs)
    return pl.pallas_call(
        kernel,
        out_shape=out_shape,
        in_specs=[pl.BlockSpec(memory_space=pltpu.SMEM) if x.ndim == 1 else IN_VMEM for x in operands],
        out_specs=specs if isinstance(out_shape, tuple) else specs[0],
        compiler_params=pltpu.CompilerParams(vmem_limit_bytes=24 << 20),
    )(*operands)


def shaped(shape, dtype=jnp.bfloat16):
    return jax.ShapeDtypeStruct(shape, dtype)


FULL = 2 * SUBLANES


def chunk_row(rank, which):
    return jnp.where(rank < FULL, which * FULL + rank, FULL + 4 * which + rank)


def route_kernel(experts, capacity, pause, ids_fwd_hbm, ids_bwd_hbm, rows_hbm, packed, targets, held, ids_fwd, ids_bwd, rows, sems):
    copies = [
        pltpu.make_async_copy(source, target, sems.at[index])
        for index, (source, target) in enumerate(((ids_fwd_hbm, ids_fwd), (ids_bwd_hbm, ids_bwd), (rows_hbm, rows)))
    ]
    for copy in copies:
        copy.start()
    for which, ids_ref in enumerate((ids_fwd, ids_bwd)):
        copies[which].wait()
        ids = ids_ref[...]
        ranks = places_in_chunks(ids, experts)
        for column in range(2):
            row = 2 * which + column
            targets[row : row + 1, :] = ids[column : column + 1] * capacity + ranks[column]
    copies[2].wait()
    pack_tiles(capacity, targets[0:1, :], targets[1:2, :], rows[...], packed)
    held[...] = lax.fori_loop(0, pause[0], lambda _, value: value * 1.0001 + 0.5, jnp.zeros(held.shape, jnp.float32))


def route_and_pack(pause, ids_fwd, ids_bwd, rows, experts, capacity):
    tokens, features = rows.shape
    in_hbm = [pltpu.with_memory_space_constraint(x, pltpu.HBM) for x in (ids_fwd, ids_bwd, rows)]
    out_shape = (tiled_shape(experts, features), shaped((4, tokens), jnp.int32), shaped((SUBLANES, LANES), jnp.float32))
    return pl.pallas_call(
        lambda *refs: route_kernel(experts, capacity, *refs),
        out_shape=out_shape,
        in_specs=[pl.BlockSpec(memory_space=pltpu.SMEM)] + [pl.BlockSpec(memory_space=pltpu.HBM)] * 3,
        out_specs=(IN_VMEM,) * 3,
        scratch_shapes=[
            pltpu.VMEM((2, tokens), jnp.int32),
            pltpu.VMEM((2, tokens), jnp.int32),
            pltpu.VMEM((tokens, features), jnp.bfloat16),
            pltpu.SemaphoreType.DMA((3,)),
        ],
        compiler_params=pltpu.CompilerParams(vmem_limit_bytes=24 << 20),
        name="route_and_pack",
    )(pause, *in_hbm)


def pair_kernel(capacity, targets, saved_rows, grad_rows, packed):
    tokens = saved_rows.shape[0]
    spots = []
    for which in range(2):
        for column in range(2):
            slot = targets[2 + column : 3 + column, :]
            expert = lax.div(slot, jnp.int32(capacity))
            spots.append(expert * (2 * capacity) + chunk_row(slot - expert * capacity, which))
    block = LANES
    for start in range(0, packed.shape[0], block):
        row = iota((block, tokens), 0) + start
        saved_hits = ones_where((row == spots[0]) | (row == spots[1]))
        grad_hits = ones_where((row == spots[2]) | (row == spots[3]))
        both = matmul(saved_hits, saved_rows[...], (1, 0)) + matmul(grad_hits, grad_rows[...], (1, 0))
        packed[start : start + block, :] = both.astype(jnp.bfloat16)


def pack_pairs(targets, saved_rows, grad_rows, experts, capacity):
    out = shaped((2 * experts * capacity, saved_rows.shape[1]))
    kernel = lambda *refs: pair_kernel(capacity, *refs)
    return call(kernel, out, targets, saved_rows, grad_rows)


def put_tiles(out_ref, tile, last_tile):
    experts, chunk_rows, lanes = out_ref.shape
    columns = (2 * chunk_rows // SUBLANES) // 5

    def put(at, value):
        rows = slice(at * SUBLANES, (at + 1) * SUBLANES)
        out_ref[:, rows, :] = value.astype(jnp.bfloat16).reshape(experts, SUBLANES, lanes)

    for part in range(2):
        for column in range(columns):
            put(part * columns + column, tile(part, column))
    for pair in range((columns + 1) // 2):
        put(2 * columns + pair, last_tile(2 * pair, min(2 * pair + 1, columns - 1)))


def chunk_tile(tiled, at):
    experts, _, lanes = tiled.shape
    return tiled[:, at * SUBLANES : (at + 1) * SUBLANES, :].reshape(experts * SUBLANES, lanes)


def tiled_shape(experts, features):
    columns = features // LANES
    return shaped((experts, (2 * columns + (columns + 1) // 2) * SUBLANES, LANES))


def pack_tiles(capacity, first, second, rows, out):
    experts = out.shape[0]
    width = experts * SUBLANES
    row = iota((width, rows.shape[0]), 0)
    chunk, within = row // SUBLANES, row % SUBLANES

    def picks(slot, allowed):
        return ones_where(((slot == first) | (slot == second)) & allowed)

    full = [matmul(picks(chunk * capacity + part * SUBLANES + within, True), rows, (1, 0)) for part in range(2)]
    last = chunk * capacity + FULL + within % 4
    early = matmul(picks(last, within < 4), rows, (1, 0))
    late = matmul(picks(last, within >= 4), rows, (1, 0))

    def lanes(column):
        return slice(column * LANES, (column + 1) * LANES)

    put_tiles(out, lambda part, c: full[part][:, lanes(c)], lambda a, b: early[:, lanes(a)] + late[:, lanes(b)])


def columns_of(weight, contract, half):
    units = 512
    span = pl.ds(pl.multiple_of(half * units, units), units)
    return weight[span, :] if contract == 1 else weight[:, span]


def hidden_kernel(core, tiled, up, away, kept):
    experts, _, lanes = tiled.shape
    columns = up.shape[0] // lanes
    width = experts * SUBLANES
    full = [jnp.concatenate([chunk_tile(tiled, p * columns + c) for c in range(columns)], axis=1) for p in range(2)]
    main = jnp.concatenate([full[p].reshape(experts, SUBLANES, -1) for p in range(2)], axis=1)
    main = main.reshape(2 * width, -1)
    lasts = [chunk_tile(tiled, 2 * columns + pair) for pair in range((columns + 1) // 2)]
    for out, half in ((away, 1 - core[0]), (kept, core[0])):
        weight = columns_of(up, 0, half)
        early = late = None
        for column in range(columns):
            part = matmul(lasts[column // 2], weight[column * lanes : (column + 1) * lanes, :], (1, 0))
            if column % 2:
                late = part if late is None else late + part
            else:
                early = part if early is None else early + part
        out[: 2 * width, :] = matmul(main, weight, (1, 0))
        out[2 * width :, :] = early + pltpu.roll(late, width - 4, 0)


def hidden_partials(core, tiled, up):
    half = shaped((3 * tiled.shape[0] * SUBLANES, up.shape[1] // 2), jnp.float32)
    return call(hidden_kernel, (half, half), core, in_vmem(tiled), in_vmem(up))


def back_kernel(core, rows, up, down_hbm, away, kept, down, sem):
    load = pltpu.make_async_copy(down_hbm, down, sem)
    load.start()
    experts, _, features = rows.shape
    full, width = experts * FULL, experts * SUBLANES
    saved = rows[:, :FULL, :].reshape(full, features)
    grads = rows[:, FULL : 2 * FULL, :].reshape(full, features)
    last = rows[:, 2 * FULL :, :].reshape(width, features)
    outs = ((away, 1 - core[0]), (kept, core[0]))
    last_hidden = []
    for out, half in outs:
        up_half = columns_of(up, 0, half)
        out[:full, :] = matmul(saved, up_half, (1, 0)).astype(out.dtype)
        last_hidden.append(matmul(last, up_half, (1, 0)))
    load.wait()
    for (out, half), hidden in zip(outs, last_hidden):
        down_half = columns_of(down, 1, half)
        out[full : 2 * full, :] = matmul(grads, down_half, (1, 1)).astype(out.dtype)
        upper = iota((width, out.shape[1]), 0) % SUBLANES < 4
        out[2 * full :, :] = jnp.where(upper, hidden, matmul(last, down_half, (1, 1))).astype(out.dtype)


def back_partials(core, rows, up, down):
    shape = (rows.shape[0] * rows.shape[1], up.shape[1] // 2)
    return pl.pallas_call(
        back_kernel,
        out_shape=(shaped(shape), shaped(shape, jnp.float32)),
        in_specs=[pl.BlockSpec(memory_space=pltpu.SMEM), IN_VMEM, IN_VMEM, pl.BlockSpec(memory_space=pltpu.HBM)],
        out_specs=(IN_VMEM, IN_VMEM),
        scratch_shapes=[pltpu.VMEM(down.shape, jnp.bfloat16), pltpu.SemaphoreType.DMA],
        compiler_params=pltpu.CompilerParams(vmem_limit_bytes=24 << 20),
        name="back_partials",
    )(core, in_vmem(rows), in_vmem(up), pltpu.with_memory_space_constraint(down, pltpu.HBM))


def slope_kernel(width, pair, came, slope):
    full = 2 * width

    def slope_of(hidden, slope_in):
        squash = 1.0 / (1.0 + jnp.exp(-hidden))
        return (slope_in * squash * (1.0 + hidden * (1.0 - squash))).astype(jnp.bfloat16)

    total = pair[...] + came[...].astype(jnp.float32)
    slope[:full, :] = slope_of(total[:full], total[full : 2 * full])
    last = total[2 * full :]
    slope[full:, :] = slope_of(last, pltpu.roll(last, width - 4, 0))


def slopes(pair, came, experts):
    out = shaped((3 * experts * SUBLANES, pair.shape[1]))
    kernel = lambda *refs: slope_kernel(experts * SUBLANES, *refs)
    return call(kernel, out, in_vmem(pair), in_vmem(came))


def results_kernel(contract, core, mine, other, weight, out):
    experts, _, lanes = out.shape
    width = experts * SUBLANES
    inner = 1 - contract
    total = matmul(mine[...], columns_of(weight, inner, core[0]), (1, contract))
    total = total + matmul(other[...], columns_of(weight, inner, 1 - core[0]), (1, contract))
    main = total[: 2 * width].reshape(experts, FULL, -1)
    last = total[2 * width :]
    moved = pltpu.roll(last, 4, 0)
    upper = iota((width, lanes), 0) % SUBLANES < 4

    def span(column):
        return slice(column * lanes, (column + 1) * lanes)

    put_tiles(
        out,
        lambda part, c: main[:, part * SUBLANES : (part + 1) * SUBLANES, span(c)],
        lambda a, b: jnp.where(upper, last[:, span(a)], moved[:, span(b)]),
    )


def tiled_results(core, mine, other, weight, contract, experts):
    out = tiled_shape(experts, weight.shape[1 - contract])
    kernel = lambda *refs: results_kernel(contract, *refs)
    return call(kernel, out, core, in_vmem(mine), in_vmem(other), in_vmem(weight))


def slot_weights(targets, route_weight, experts, capacity):
    tokens = targets.shape[1]
    width = experts * SUBLANES
    expert, rank = targets // capacity, targets % capacity
    options = []
    for odd in range(2):
        last = 2 * width + expert * SUBLANES + (rank - FULL) + 4 * odd
        main = (rank // SUBLANES) * width + expert * SUBLANES + rank % SUBLANES
        options.append(jnp.where(rank < FULL, main, last))
    spots = jnp.stack(options)
    bytes_of = jnp.stack((route_weight // 256, route_weight % 256))
    labels = jnp.arange(3 * width, dtype=jnp.int32)
    hit = spots[:, :, :, None] == labels
    chosen = jnp.where(hit[:, None], bytes_of[None, :, :, :, None], 0).sum(axis=2)
    return chosen.astype(jnp.bfloat16).reshape(2, 2 * tokens, 3 * width)


def mix_kernel(weights, back, rows, out):
    tokens, features = rows.shape
    columns = features // LANES
    for column in range(columns):
        spots = (column, columns + column, 2 * columns + column // 2)
        tile = jnp.concatenate([chunk_tile(back, at) for at in spots], axis=0)
        both = matmul(weights[column % 2], tile, (1, 0))
        summed = (both[:tokens] * 256.0 + both[tokens:]) * (1.0 / 32768.0)
        lanes = slice(column * LANES, (column + 1) * LANES)
        out[:, lanes] = (rows[:, lanes].astype(jnp.float32) + summed).astype(jnp.bfloat16)


def mix(weights, back, rows):
    return call(mix_kernel, shaped(rows.shape), in_vmem(weights), in_vmem(back), in_vmem(rows))


def land_kernel(source, target, sem):
    copy = pltpu.make_async_copy(source, target, sem)
    copy.start()
    copy.wait()


def land(rows):
    in_hbm = pl.BlockSpec(memory_space=pltpu.HBM)
    return pl.pallas_call(
        land_kernel,
        out_shape=shaped(rows.shape),
        in_specs=[in_hbm],
        out_specs=in_hbm,
        scratch_shapes=[pltpu.SemaphoreType.DMA],
        name="land",
    )(pltpu.with_memory_space_constraint(rows, pltpu.HBM))


def exchange(chunks):
    return lax.all_to_all(chunks, "expert", split_axis=0, concat_axis=0, tiled=True)


def swapped(value, mask):
    count = lax.axis_size("shard")
    return lax.ppermute(value, "shard", [(source, source ^ mask) for source in range(count)])


def rounded(value):
    return value.astype(jnp.bfloat16)


def from_behind(value, axis, steps):
    count = lax.axis_size(axis)
    pairs = [(source, (source + steps) % count) for source in range(count)]
    return lax.ppermute(value, axis, pairs)


def matmul(a, b, contract):
    return lax.dot_general(a, b, ((contract[:1], contract[1:]), ((), ())), preferred_element_type=jnp.float32)


def per_device(fwd_in, saved_in, grad_in, w_in, w_out, ids_fwd, weight_fwd, ids_bwd, weight_bwd):
    peers = lax.axis_size("expert")
    core = (lax.axis_index("shard") % 2).reshape(1)
    tok_count, features = fwd_in.shape[1:]
    slot_count = ids_fwd.shape[2]
    capacity = max(2, (tok_count * slot_count * 5 + 4 * peers - 1) // (4 * peers))
    up, down = w_in[0, 0], w_out[0, 0]
    fwd_rows, saved_rows, grad_rows = fwd_in[0], saved_in[0], grad_in[0]

    fwd_packed, targets, _ = route_and_pack(core * PAUSE, ids_fwd[0].T, ids_bwd[0].T, fwd_rows, peers, capacity)
    fwd_got = exchange(fwd_packed)
    bwd_packed = pack_pairs(targets, saved_rows, grad_rows, peers, capacity)
    fwd_weights = slot_weights(targets[:2], weight_fwd[0].T, peers, capacity)
    bwd_weights = slot_weights(targets[2:], weight_bwd[0].T, peers, capacity)
    bwd_got = exchange(bwd_packed.reshape(peers, 2 * capacity, features))

    away, kept = hidden_partials(core, fwd_got, up)
    pair = kept + swapped(away, 1)
    hidden = pair + swapped(rounded(pair), 2).astype(jnp.float32)
    active = rounded(jax.nn.silu(hidden))
    other_active = swapped(active, 1)
    fwd_results = tiled_results(core, active, other_active, down, 0, peers)
    fwd_back = exchange(fwd_results)

    back_away, back_kept = back_partials(core, bwd_got, up, down)
    back_pair = back_kept + swapped(back_away, 1).astype(jnp.float32)
    back_came = swapped(rounded(back_pair), 2)
    slope = slopes(back_pair, back_came, peers)
    other_slope = swapped(slope, 1)
    bwd_results = tiled_results(core, slope, other_slope, up, 1, peers)
    bwd_back = exchange(bwd_results)

    layer_out = mix(fwd_weights, fwd_back, fwd_rows)
    fwd_out = from_behind(layer_out, "section", 1)
    fwd_out = land(fwd_out)
    layer_grad = mix(bwd_weights, bwd_back, grad_rows)
    bwd_out = from_behind(layer_grad, "section", -1)
    return (fwd_out[None], bwd_out[None])


def solution(mesh):
    rows = P("section", "expert", "shard")
    slots = P("section", "expert", None)
    in_specs = (
        rows,
        rows,
        rows,
        P("section", "expert", "shard", None),
        P("section", "expert", None, "shard"),
        slots,
        slots,
        slots,
        slots,
    )
    return jax.shard_map(per_device, mesh=mesh, in_specs=in_specs, out_specs=(rows, rows), check_vma=False)
```
